32 devices in a mesh: col: 4 (over z), row: 8 (over y, x, core).
Axes of the slice: x: 2, y: 2, z: 4, core: 2. Of those that a mesh axis runs over, the one named last changes fastest.
Arguments:
- queries: bfloat16 [32768, 256], P(('col', 'row')), may hold values from -6 to 6
- keys: bfloat16 [32768, 256], P(('col', 'row')), may hold values from -6 to 6
- values: bfloat16 [32768, 256], P(('col', 'row')), may hold values from -6 to 6
- out_grad: bfloat16 [32768, 256], P(('col', 'row')), may hold values from -6 to 6
- weight_table: float32 [64, 2, 21], replicated, may hold values from 0.25 to 2
- profile: int32 [32768], P(('col', 'row')), may hold values from 0 to 63
Outputs:
- output: float32 [32768, 256], P(('col', 'row'))
- query_grad: float32 [32768, 256], P(('col', 'row'))
- key_grad: float32 [32768, 256], P(('col', 'row'))
- value_grad: float32 [32768, 256], P(('col', 'row'))
The draws below stay inside these ranges and needn't reach their ends.
All inputs are finite; a program needn't handle non-finite values.
Results may differ from the reference program's by a relative error of at most 0.0034.
Values sent between devices are 32-bit elements; how exact they have to be, the bound alone decides.
A program may use at most 128 MiB of HBM per device.

```python
import math
import jax
import jax.numpy as jnp
from jax import lax

H = 2
DH = 128
LEVELS = 21
PROFILES = 64
SEQ = 32768
N_COL = 4
N_ROW = 8


def with_ends(array, own_key, smallest, high):
    shape = array.shape
    spot = [jax.random.randint(jax.random.fold_in(own_key, axis), (), 0, shape[axis]) for axis in range(len(shape))]
    array = array.at[tuple(spot)].set(smallest)
    longest = shape.index(max(shape))
    spot[longest] = (spot[longest] + 1) % shape[longest]
    return array.at[tuple(spot)].set(high)


def shard_levels(key, extent, split, low, largest):
    def one(position, shards_of):
        steps = jax.random.uniform(jax.random.fold_in(jax.random.fold_in(key, 6), position), (shards_of,), jnp.float32, low / len(split), largest / len(split))
        return jnp.repeat(jnp.exp(steps), extent[position] // shards_of).reshape((-1,) + (1,) * (len(extent) - position - 1))

    gain = one(*split[0])
    for cut in split[1:]:
        gain = gain * one(*cut)
    return gain


def scatter_about(rng, dims, scale, most, shards=(), kind=jnp.bfloat16):
    array = scale * jax.random.normal(rng, dims, jnp.float32)
    if shards:
        array = array * shard_levels(rng, dims, shards, -0.22, 0.18)
    return jnp.clip(array, -most, most).astype(kind)


def setup_inputs(seed: int = 0) -> dict:
    key_of = jax.random.split(jax.random.key(seed), 7)
    return {
        "queries": scatter_about(key_of[0], (SEQ, H * DH), 1.0, 6.0, ((0, 32),)),
        "keys": scatter_about(key_of[1], (SEQ, H * DH), 1.0, 6.0, ((0, 32),)),
        "values": scatter_about(key_of[2], (SEQ, H * DH), 1.0, 6.0, ((0, 32),)),
        "out_grad": scatter_about(key_of[3], (SEQ, H * DH), 1.0, 6.0, ((0, 32),)),
        "weight_table": jnp.clip(jnp.exp(jax.random.uniform(key_of[4], (PROFILES, H, LEVELS), jnp.float32, math.log(0.25), math.log(2.0))), 0.25, 2.0),
        "profile": with_ends(jax.random.randint(key_of[5], (SEQ,), 0, PROFILES), jax.random.fold_in(key_of[5], 1), 0, PROFILES - 1).astype(jnp.int32),
    }


HIGHEST_PRECISION = lax.Precision.HIGHEST

def digit_count(numbers, count):
    total = jnp.zeros_like(numbers)
    for digit_place in range(count):
        total = total + (numbers >= 1 << digit_place).astype(jnp.int32)
    return total

def level_weights(weight_table, profile, head_width):
    table_rows = weight_table.shape[0]
    onehot = (profile[:, None] == jnp.arange(table_rows, dtype=jnp.int32)[None, :]).astype(jnp.float32)
    flat_table = weight_table.reshape(table_rows, -1)
    picked = jnp.dot(onehot, flat_table, precision=HIGHEST_PRECISION, preferred_element_type=jnp.float32)
    picked = picked.reshape(profile.shape[0], weight_table.shape[1], weight_table.shape[2])
    depth = jnp.arange(weight_table.shape[2], dtype=jnp.float32)
    scaling = jnp.exp2(-0.5 * depth) / math.sqrt(head_width)
    return picked * scaling

def sibling_sums(states, bit_place, receiver):
    count = states.shape[0]
    remain = states.shape[1:]
    shape = (count >> bit_place + 1, 2, 1 << bit_place) + remain
    grouped = lax.optimization_barrier(jnp.sum(states.reshape(shape), axis=2))
    source = grouped[:, 1 - receiver]
    empty = jnp.zeros_like(source)
    halves = [source, empty] if receiver == 0 else [empty, source]
    paired = jnp.stack(halves, axis=1)
    spread = jnp.broadcast_to(paired[:, :, None], shape)
    return spread.reshape(states.shape)

def tile_local(query_heads, key_heads, value_heads, grad_heads, weights, tile_bits):
    count = query_heads.shape[0]
    places = jnp.arange(count, dtype=jnp.int32)
    levels = digit_count(jnp.bitwise_xor(places[:, None], places[None, :]), tile_bits)
    causal = places[None, :] <= places[:, None]
    level_mask = jnp.zeros((query_heads.shape[1], count, count), jnp.float32)
    for level in range(tile_bits + 1):
        level_mask = level_mask + jnp.where(levels[None] == level, jnp.transpose(weights[:, :, level])[:, :, None], 0.0)
    level_mask = jnp.where(causal[None], level_mask, 0.0)
    query_f = query_heads.astype(jnp.float32)
    key_f = key_heads.astype(jnp.float32)
    value_f = value_heads.astype(jnp.float32)
    grad_f = grad_heads.astype(jnp.float32)
    scores = jnp.einsum('thd,shd->hts', query_f, key_f, precision=HIGHEST_PRECISION)
    local_probs = (scores * level_mask).astype(jnp.bfloat16)
    probs_f = local_probs.astype(jnp.float32)
    local_out = jnp.einsum('hts,she->the', probs_f, value_f, precision=HIGHEST_PRECISION)
    grad_scores = jnp.einsum('the,she->hts', grad_f, value_f, precision=HIGHEST_PRECISION)
    local_grad = (grad_scores * level_mask).astype(jnp.bfloat16).astype(jnp.float32)
    local_dq = jnp.einsum('hts,shd->thd', local_grad, key_f, precision=HIGHEST_PRECISION)
    local_dk = jnp.einsum('hts,thd->shd', local_grad, query_f, precision=HIGHEST_PRECISION)
    local_dv = jnp.einsum('hts,the->she', probs_f, grad_f, precision=HIGHEST_PRECISION)
    return (local_out, local_dq, local_dk, local_dv)

def tile_far(query_heads, key_heads, value_heads, grad_heads, far_weights, bucket_half, pulled_half):
    query_f = query_heads.astype(jnp.float32)
    key_f = key_heads.astype(jnp.float32)
    value_f = value_heads.astype(jnp.float32)
    grad_f = grad_heads.astype(jnp.float32)
    bucket_f = bucket_half.astype(jnp.float32)
    pulled_f = pulled_half.astype(jnp.float32)
    reach = jnp.einsum('thd,lhde->thle', query_f, bucket_f, precision=HIGHEST_PRECISION)
    far_out = lax.optimization_barrier(jnp.sum(reach * far_weights[..., None], axis=2))
    back = jnp.einsum('the,lhde->thld', grad_f, bucket_f, precision=HIGHEST_PRECISION)
    far_dq = lax.optimization_barrier(jnp.sum(back * far_weights[..., None], axis=2))
    far_dk = jnp.einsum('the,hde->thd', value_f, pulled_f, precision=HIGHEST_PRECISION)
    far_dv = jnp.einsum('thd,hde->the', key_f, pulled_f, precision=HIGHEST_PRECISION)
    return (far_out, far_dq, far_dk, far_dv)

def tile_grad_state(query_heads, grad_heads, far_weights):
    weighted = (query_heads.astype(jnp.float32)[:, :, None, :] * far_weights[..., None]).astype(jnp.bfloat16)
    return jnp.einsum('thld,the->lhde', weighted.astype(jnp.float32), grad_heads.astype(jnp.float32), precision=HIGHEST_PRECISION)

def reference(queries, keys, values, out_grad, weight_table, profile):
    tile_count = N_COL * N_ROW
    token_count = queries.shape[0] // tile_count
    head_count = weight_table.shape[1]
    head_width = queries.shape[1] // head_count
    tile_bits = token_count.bit_length() - 1
    far_levels = tile_count.bit_length() - 1
    weights = level_weights(weight_table, profile, head_width).reshape(tile_count, token_count, head_count, -1)
    far_weights = weights[:, :, :, tile_bits + 1:tile_bits + 1 + far_levels]
    tile_shape = (tile_count, token_count, head_count, head_width)
    query_tiles = queries.reshape(tile_shape)
    key_tiles = keys.reshape(tile_shape)
    value_tiles = values.reshape(tile_shape)
    grad_tiles = out_grad.reshape(tile_shape)
    tile_state = jnp.einsum('bthd,bthe->bhde', key_tiles.astype(jnp.float32), value_tiles.astype(jnp.float32), precision=HIGHEST_PRECISION)

    def grad_of_tile(items):
        return tile_grad_state(items[0], items[1], items[2])
    grad_state = lax.map(grad_of_tile, (query_tiles, grad_tiles, far_weights))
    bucket = jnp.stack([sibling_sums(tile_state, level, 1) for level in range(far_levels)], axis=1)
    bucket_half = bucket.astype(jnp.bfloat16)
    pulled = jnp.zeros_like(tile_state)
    for level in range(far_levels):
        pulled = pulled + sibling_sums(grad_state[:, level], level, 0)
    pulled_half = pulled.astype(jnp.bfloat16)

    def per_tile(items):
        query_heads, key_heads, value_heads, grad_heads, tile_weights, bucket_tile, pulled_tile = items
        local_out, local_dq, local_dk, local_dv = tile_local(query_heads, key_heads, value_heads, grad_heads, tile_weights, tile_bits)
        far_out, far_dq, far_dk, far_dv = tile_far(query_heads, key_heads, value_heads, grad_heads, tile_weights[:, :, tile_bits + 1:tile_bits + 1 + far_levels], bucket_tile, pulled_tile)
        return (local_out + far_out, local_dq + far_dq, local_dk + far_dk, local_dv + far_dv)
    results = lax.map(per_tile, (query_tiles, key_tiles, value_tiles, grad_tiles, weights, bucket_half, pulled_half))
    return (results[0].reshape(queries.shape), results[1].reshape(queries.shape), results[2].reshape(queries.shape), results[3].reshape(queries.shape))
```

```python
import functools
import math

import jax
import jax.numpy as jnp
from jax import lax
from jax.experimental import pallas as pl
from jax.experimental.pallas import tpu as pltpu
from jax.sharding import PartitionSpec as P

MESH = pl.DeviceIdType.MESH
F32 = jnp.float32
BF16 = jnp.bfloat16
NN = (((1,), (0,)), ((), ()))
NT = (((1,), (1,)), ((), ()))
TN = (((0,), (0,)), ((), ()))
CHUNK = 128


def mm(a, b, dims):
    return lax.dot_general(a, b, dims, preferred_element_type=F32)


def main_kernel(
    dims,
    q_ref, k_ref, v_ref, g_ref, tab_ref, prof_ref,
    lo_ref, lq_ref, lk_ref, lv_ref, wq_ref, wg_ref, bnt_ref, bnn_ref, pul_ref,
    w_scr, lev_scr, m_scr, p_scr, d_scr,
    st, x0, pin, sum1, ain, b1, b2, tot, zout, zin, far,
    pair_send, pair_recv, red_send, red_recv, z_send, z_recv, ga_send, ga_recv, gb_send, gb_recv,
):
    T, H, D, cols, rows, span = dims
    rows_bits = rows.bit_length() - 1
    col_bits = cols.bit_length() - 1
    L = rows_bits + col_bits
    chips = rows // 2
    qb = rows_bits - 1
    R = D // chips
    tile_bits = T.bit_length() - 1
    span_bits = span.bit_length() - 1
    z = lax.axis_index("col")
    row = lax.axis_index("row")
    core = lax.rem(row, 2)
    chip = lax.div(row, 2)
    other = 1 - core

    def chip_at(offset):
        return lax.rem(chip + offset, chips)

    def col_at(offset):
        return lax.rem(z + offset, cols)

    barrier = pltpu.get_barrier_semaphore()
    pl.semaphore_signal(barrier, inc=1, device_id=(z, chip * 2 + other), device_id_type=MESH)
    for offset in range(1, chips):
        pl.semaphore_signal(
            barrier, inc=1, device_id=(z, chip_at(offset) * 2 + core), device_id_type=MESH
        )
    for offset in range(1, cols):
        pl.semaphore_signal(barrier, inc=1, device_id=(col_at(offset), row), device_id_type=MESH)

    def remote(src, dst, send, recv, device):
        return pltpu.make_async_remote_copy(
            src_ref=src, dst_ref=dst, send_sem=send, recv_sem=recv,
            device_id=device, device_id_type=MESH,
        )

    profiles = tab_ref.shape[0]
    levels = tab_ref.shape[2]
    onehot = jnp.where(
        lax.broadcasted_iota(jnp.int32, (profiles, T), 0) == prof_ref[...], 1.0, 0.0
    ).astype(BF16)
    onehot = jnp.concatenate([onehot, onehot, onehot], axis=0)
    place = lax.broadcasted_iota(jnp.int32, (profiles, levels), 1)
    scale = jnp.zeros((profiles, levels), F32)
    for level in range(levels):
        scale = jnp.where(place == level, 2.0 ** (-0.5 * level) / math.sqrt(D), scale)
    for h in range(H):
        table = tab_ref[:, h, :] * scale
        top = table.astype(BF16)
        rest = table - top.astype(F32)
        mid = rest.astype(BF16)
        low = (rest - mid.astype(F32)).astype(BF16)
        w_scr[h] = mm(onehot, jnp.concatenate([top, mid, low], axis=0), TN)

    def weigh(src, dst, h):
        for start in range(0, T, CHUNK):
            rs = slice(start, start + CHUNK)
            x = src[rs, h * D : (h + 1) * D].astype(F32)
            for j in range(L):
                level = tile_bits + 1 + j
                c = (h * L + j) * D
                dst[rs, c : c + D] = (x * w_scr[h, rs, level : level + 1]).astype(BF16)

    for h in range(H):
        hs = slice(h * D, (h + 1) * D)
        weigh(q_ref, wq_ref, h)
        state = mm(v_ref[:, hs], k_ref[:, hs], TN)
        grads = mm(g_ref[:, hs], wq_ref[:, h * L * D : (h + 1) * L * D], TN)
        st[h, 0] = state
        for j in range(1, L):
            st[h, j] = grads[:, j * D : (j + 1) * D]
        x0[h] = jnp.where(core == 0, state, grads[:, :D])

    pl.semaphore_wait(barrier, chips + cols - 1)
    partner = (z, chip * 2 + other)
    pair = remote(st.at[other], pin, pair_send.at[0], pair_recv.at[0], partner)
    pair.start()
    near = remote(x0, far.at[0], pair_send.at[1], pair_recv.at[1], partner)
    near.start()

    r_at = lax.broadcasted_iota(jnp.int32, (span, span), 0)
    c_at = lax.broadcasted_iota(jnp.int32, (span, span), 1)
    apart = jnp.bitwise_xor(r_at, c_at)
    lev = jnp.zeros((span, span), jnp.int32)
    for bit in range(span_bits):
        lev = lev + jnp.where(apart >= 1 << bit, 1, 0)
    lev_scr[...] = jnp.where(c_at <= r_at, lev, -1)

    last = T // span - 1

    def unit(h, i):
        hs = slice(h * D, (h + 1) * D)
        ts = slice(i * span, (i + 1) * span)
        width = (i + 1) * span
        for start in range(0, span, 64):
            rs = slice(start, start + 64)
            wts = slice(i * span + start, i * span + start + 64)
            mask = jnp.zeros((64, span), F32)
            here = lev_scr[rs, :]
            for level in range(span_bits + 1):
                mask = jnp.where(here == level, w_scr[h, wts, level : level + 1], mask)
            m_scr[rs, :] = mask
        q = q_ref[ts, hs]
        g = g_ref[ts, hs]
        for b in range(i + 1):
            bs = slice(b * span, (b + 1) * span)
            if b < i:
                level = span_bits + (b ^ i).bit_length()
                mask = w_scr[h, ts, level : level + 1]
            else:
                mask = m_scr[...]
            p_scr[:, bs] = (mm(q, k_ref[bs, hs], NT) * mask).astype(BF16)
            d_scr[:, bs] = (mm(g, v_ref[bs, hs], NT) * mask).astype(BF16)
        ws = slice(0, width)
        lo_ref[ts, hs] = mm(p_scr[:, ws], v_ref[ws, hs], NN)
        lq_ref[ts, hs] = mm(d_scr[:, ws], k_ref[ws, hs], NN)
        dk = mm(d_scr[:, ws], q, TN)
        dv = mm(p_scr[:, ws], g, TN)
        if i == last:
            lk_ref[ws, hs] = dk
            lv_ref[ws, hs] = dv
        else:
            lk_ref[ws, hs] += dk
            lv_ref[ws, hs] += dv

    work = [(h, i) for i in range(last, -1, -1) for h in range(H)]
    cut1 = 1
    cut2 = max(cut1, len(work) * 4 // 8)
    cut3 = max(cut2, len(work) * 6 // 8)

    for h, i in work[:cut1]:
        unit(h, i)

    pair.wait()
    for p in range(chips):
        rs = slice(p * R, (p + 1) * R)
        sum1[p] = st[core, :, rs, :] + pin[:, rs, :]
    reduces = []
    for offset in range(1, chips):
        to = chip_at(offset)
        copy = remote(
            sum1.at[to], ain.at[chip], red_send.at[offset], red_recv.at[offset],
            (z, to * 2 + core),
        )
        copy.start()
        reduces.append(copy)
    ain[chip] = sum1[chip]

    for h, i in work[cut1:cut2]:
        unit(h, i)

    for copy in reduces:
        copy.wait()
    tot[0] = sum([ain[p, 0] for p in range(1, chips)], ain[0, 0])
    for jj in range(col_bits):
        tot[1 + jj] = sum([ain[p, 1 + qb + jj] for p in range(1, chips)], ain[0, 1 + qb + jj])

    def sibling(mine, theirs, bit):
        same = lax.div(mine, 2 << bit) == theirs >> bit + 1
        differs = lax.rem(lax.div(mine, 1 << bit), 2) != theirs >> bit & 1
        return jnp.logical_and(same, differs)

    for to in range(cols):
        value = jnp.zeros((R, D), F32)
        for jj in range(col_bits):
            piece = tot[0] if to >> jj & 1 else tot[1 + jj]
            value = jnp.where(sibling(z, to, jj), piece, value)
        zout[to] = value
    crosses = []
    for offset in range(1, cols):
        to = col_at(offset)
        copy = remote(
            zout.at[to], zin.at[z], z_send.at[offset], z_recv.at[offset], (to, row)
        )
        copy.start()
        crosses.append(copy)
    zin[z] = jnp.zeros((R, D), F32)

    mine = pl.ds(pl.multiple_of(chip * R, R), R)
    firsts = []
    if qb:
        for to in range(chips):
            for jj in range(qb):
                source = 0 if to >> jj & 1 else 1 + jj
                group = [
                    p for p in range(chips)
                    if p >> jj + 1 == to >> jj + 1 and (p >> jj & 1) != (to >> jj & 1)
                ]
                b1[to, jj] = sum([ain[p, source] for p in group[1:]], ain[group[0], source])
        for offset in range(1, chips):
            to = chip_at(offset)
            copy = remote(
                b1.at[to], far.at[pl.ds(1, qb), core, mine], ga_send.at[offset],
                ga_recv.at[offset], (z, to * 2 + core),
            )
            copy.start()
            firsts.append(copy)
        for jj in range(qb):
            far[1 + jj, core, mine] = b1[chip, jj]

    for h, i in work[cut2:cut3]:
        unit(h, i)

    for copy in crosses:
        copy.wait()
    for jj in range(col_bits):
        value = jnp.zeros((R, D), F32)
        for source in range(cols):
            value = value + jnp.where(sibling(z, source, jj), zin[source], 0.0)
        b2[jj] = value
    seconds = []
    if col_bits:
        for offset in range(1, chips):
            to = chip_at(offset)
            copy = remote(
                b2, far.at[pl.ds(1 + qb, col_bits), core, mine], gb_send.at[offset],
                gb_recv.at[offset], (z, to * 2 + core),
            )
            copy.start()
            seconds.append(copy)
        for jj in range(col_bits):
            far[1 + qb + jj, core, mine] = b2[jj]
    relays = []
    if qb:
        for copy in firsts:
            copy.wait()
        relay = remote(
            far.at[pl.ds(1, qb), core], far.at[pl.ds(1, qb), core],
            pair_send.at[2], pair_recv.at[2], partner,
        )
        relay.start()
        relays.append(relay)

    for h, i in work[cut3:]:
        unit(h, i)
    for h in range(H):
        weigh(g_ref, wg_ref, h)

    if col_bits:
        for copy in seconds:
            copy.wait()
        relay = remote(
            far.at[pl.ds(1 + qb, col_bits), core], far.at[pl.ds(1 + qb, col_bits), core],
            pair_send.at[3], pair_recv.at[3], partner,
        )
        relay.start()
        relays.append(relay)
    near.wait()
    for relay in relays:
        relay.wait()

    digits = [core]
    digits += [lax.rem(lax.div(chip, 1 << jj), 2) for jj in range(qb)]
    digits += [lax.rem(lax.div(z, 1 << jj), 2) for jj in range(col_bits)]
    for h in range(H):
        pulled = jnp.zeros((D, D), F32)
        for j in range(L):
            value = far[j, h]
            up = digits[j] == 1
            pulled = pulled + jnp.where(up, 0.0, value)
            half = jnp.where(up, value, 0.0).astype(BF16)
            bnt_ref[h, :, j * D : (j + 1) * D] = half
            bnn_ref[h, j * D : (j + 1) * D, :] = half
        pul_ref[h] = pulled.astype(BF16)


def finish_kernel(
    dims, lo, lq, lk, lv, wq, wg, k, v, bnt, bnn, pul, out, dq, dk, dv
):
    H, D, L = dims
    for h in range(H):
        hs = slice(h * D, (h + 1) * D)
        ls = slice(h * L * D, (h + 1) * L * D)
        out[:, hs] = lo[:, hs] + mm(wq[:, ls], bnt[h], NT)
        dq[:, hs] = lq[:, hs] + mm(wg[:, ls], bnn[h], NN)
        dk[:, hs] = lk[:, hs] + mm(v[:, hs], pul[h], NN)
        dv[:, hs] = lv[:, hs] + mm(k[:, hs], pul[h], NT)


def shards(cols, rows, queries, keys, values, out_grad, weight_table, profile):
    T = queries.shape[0]
    H = weight_table.shape[1]
    D = queries.shape[1] // H
    levels = weight_table.shape[2]
    L = rows.bit_length() + cols.bit_length() - 2
    chips = rows // 2
    qb = rows.bit_length() - 2
    col_bits = cols.bit_length() - 1
    R = D // chips
    span = min(T, 256)
    assert H == 2 and R % 8 == 0
    vm = pl.BlockSpec(memory_space=pltpu.VMEM)
    sds = jax.ShapeDtypeStruct
    dma = pltpu.SemaphoreType.DMA
    local = sds((T, H * D), F32)
    weighted = sds((T, H * L * D), BF16)
    parts = pl.pallas_call(
        functools.partial(main_kernel, (T, H, D, cols, rows, span)),
        out_shape=[
            local, local, local, local, weighted, weighted,
            sds((H, D, L * D), BF16), sds((H, L * D, D), BF16), sds((H, D, D), BF16),
        ],
        in_specs=[vm] * 6,
        out_specs=[vm] * 9,
        scratch_shapes=[
            pltpu.VMEM((H, T, levels), F32),
            pltpu.VMEM((span, span), jnp.int32),
            pltpu.VMEM((span, span), F32),
            pltpu.VMEM((span, T), BF16),
            pltpu.VMEM((span, T), BF16),
            pltpu.VMEM((H, L, D, D), F32),
            pltpu.VMEM((H, D, D), F32),
            pltpu.VMEM((L, D, D), F32),
            pltpu.VMEM((chips, L, R, D), F32),
            pltpu.VMEM((chips, L, R, D), F32),
            pltpu.VMEM((chips, max(qb, 1), R, D), F32),
            pltpu.VMEM((max(col_bits, 1), R, D), F32),
            pltpu.VMEM((1 + col_bits, R, D), F32),
            pltpu.VMEM((cols, R, D), F32),
            pltpu.VMEM((cols, R, D), F32),
            pltpu.VMEM((L, H, D, D), F32),
            dma((4,)), dma((4,)),
            dma((chips,)), dma((chips,)),
            dma((cols,)), dma((cols,)),
            dma((chips,)), dma((chips,)),
            dma((chips,)), dma((chips,)),
        ],
        compiler_params=pltpu.CompilerParams(
            collective_id=0, has_side_effects=True, vmem_limit_bytes=40 * 1024 * 1024
        ),
        name="main",
    )(queries, keys, values, out_grad, weight_table, profile.reshape(1, T))
    lo, lq, lk, lv, wq, wg, bnt, bnn, pul = parts
    block = min(T, 256)
    tile = pl.BlockSpec((block, H * D), lambda i: (i, 0))
    wide = pl.BlockSpec((block, H * L * D), lambda i: (i, 0))
    whole = lambda s: pl.BlockSpec(s, lambda i: (0, 0, 0))
    return pl.pallas_call(
        functools.partial(finish_kernel, (H, D, L)),
        grid=(T // block,),
        out_shape=[local] * 4,
        in_specs=[tile] * 4 + [wide] * 2 + [tile] * 2
        + [whole((H, D, L * D)), whole((H, L * D, D)), whole((H, D, D))],
        out_specs=[tile] * 4,
        compiler_params=pltpu.CompilerParams(vmem_limit_bytes=24 * 1024 * 1024),
        name="finish",
    )(lo, lq, lk, lv, wq, wg, keys, values, bnt, bnn, pul)


def solution(mesh):
    tokens = P(("col", "row"), None)
    return jax.shard_map(
        functools.partial(shards, mesh.shape["col"], mesh.shape["row"]),
        mesh=mesh,
        in_specs=(tokens,) * 4 + (P(), P(("col", "row"))),
        out_specs=(tokens,) * 4,
        check_vma=False,
    )
```
